256 devices in a mesh: rows: 64 (over x, z_hi, y, core), feat: 4 (over z_lo).
Axes of the slice: x: 4, y: 4, z: 8 (z_hi: 2, z_lo: 4; z = z_hi * 4 + z_lo), core: 2. Of those that a mesh axis runs over, the one named last changes fastest.
Arguments:
- bins: int32 [65536, 512], P('rows', 'feat'), may hold values from -2147483648 to 2147483647, as said below
- hessian: float32 [262144], P('rows'), may hold values from 0.05 to 1
- thresholds: float32 [128], replicated, may hold values from 0.02 to 0.98
Outputs:
- cuts: float32 [512, 128], P('feat')
The draws below stay inside these ranges and needn't reach their ends.
Inputs may be any that keep to these rules, and one draw needn't show every extreme that they name: `bins`: each word holds the bin ids, 0 to 255, of rows 4i to 4i + 3 of one feature, row 4i + k in bits 8k to 8k + 7 of the two's complement word.
All inputs are finite; a program needn't handle non-finite values.
Results may differ from the reference program's by a relative error of at most 0.000065.
Values sent between devices are 32-bit elements; how exact they have to be, the bound alone decides.
A program may use at most 192 MiB of HBM per device.

```python
import math
import jax
import jax.numpy as jnp

F = 512
BINS = 256
Q = 128
ROW_DEV = 4096
ROWS = 262144
N_ROWS = 64


def draw_bins(key, part):
    key = jax.random.fold_in(key, 17)
    first, second, third, fourth = jax.random.split(key, 4)
    spread = jax.random.randint(first, (ROWS, F), 0, BINS)
    centers = jax.random.randint(second, (N_ROWS, F), 0, BINS)
    offsets = jax.random.randint(third, (ROWS, F), 0, 8)
    banded = jax.random.randint(fourth, (ROWS, F), 0, 2) == 0
    owner = jnp.arange(ROWS, dtype=jnp.int32) // ROW_DEV
    center_rows = centers[owner]
    ids = jnp.where(banded, (center_rows + offsets) % BINS, spread).astype(jnp.int32)
    grouped = ids.reshape(ROWS // 4, 4, F)
    packed = jnp.zeros((ROWS // 4, F), jnp.int32)
    for k in range(4):
        packed = jnp.bitwise_or(packed, jnp.left_shift(grouped[:, k, :], 8 * k))
    return packed.astype(jnp.int32)


def block_levels(own_key, dims, pieces, least, largest):
    loudness = 1.0
    for dim, shards_of in pieces:
        heights = jax.random.uniform(jax.random.fold_in(jax.random.fold_in(own_key, 6), dim), (shards_of,), jnp.float32, least / len(pieces), largest / len(pieces))
        loudness = loudness * jnp.repeat(jnp.exp(heights), dims[dim] // shards_of).reshape((-1,) + (1,) * (len(dims) - 1 - dim))
    return loudness


def setup_inputs(seed: int = 0) -> dict:
    key_list = jax.random.split(jax.random.key(seed), 4)
    return {
        "bins": draw_bins(jax.random.fold_in(key_list[3], 71), 0),
        "hessian": jnp.clip(jnp.exp(math.log(1.0) - 2.9957323 * jax.random.uniform(key_list[1], (ROWS,), jnp.float32) ** block_levels(key_list[1], (ROWS,), ((0, 64),), -0.2, 0.2)), 0.05, 1.0),
        "thresholds": jnp.clip(jax.random.uniform(key_list[2], (Q,), jnp.float32, 0.02, 0.98), 0.02, 0.98),
    }


def unpack(words):
    parts = [jnp.bitwise_and(jnp.right_shift(words, 8 * k), 255) for k in range(4)]
    stacked = jnp.stack(parts, axis=1)
    return stacked.reshape(words.shape[0] * 4, words.shape[1]).astype(jnp.int32)


def cut_positions(hist, thresholds):
    cum = jnp.cumsum(hist, axis=1)
    before = cum - hist
    total = cum[:, -1]
    target = thresholds[None, :, None] * total[:, None, None]
    ratio = (target - before[:, None, :]) / (hist[:, None, :] + 1.0)
    return jnp.sum(jnp.clip(ratio, 0.0, 1.0), axis=2)


def reference(bins, hessian, thresholds):
    ids = unpack(bins)

    def one_feature(column):
        return jax.ops.segment_sum(hessian, column, num_segments=BINS)

    hist = jax.vmap(one_feature)(ids.T).astype(jnp.float32)
    return cut_positions(hist, thresholds)
```

```python
import functools

import jax
import jax.numpy as jnp
import numpy as np
from jax import lax
from jax.experimental import pallas as pl
from jax.experimental.pallas import tpu as pltpu
from jax.sharding import PartitionSpec as P

OFFSETS = sorted(
    ((dx, dy) for dx in range(4) for dy in range(4)),
    key=lambda o: -(min(o[0], 4 - o[0]) + min(o[1], 4 - o[1])),
)
BARRIER_STEP = 3


def row_of(x, z, y, core):
    return ((x * 2 + z) * 4 + y) * 2 + core


def digit_patterns():
    r = lax.broadcasted_iota(jnp.int32, (16, 128), 0)
    low = [[((r + 16 * p) << (8 * b)).astype(jnp.int16) for p in range(2)] for b in range(2)]
    high = [((r % 8) << (5 + 8 * b)).astype(jnp.int16) for b in range(2)]
    return low, high


def spread_weights(h_ref, pieces_ref):
    lane = lax.broadcasted_iota(jnp.int32, (8, 128), 1)
    parts = [h_ref[pl.ds(s, 8, stride=4), :] for s in range(4)]
    for k in range(4):
        index = (lane % 32) * 4 + k
        rows = jnp.zeros((8, 128), jnp.float32)
        for s in range(4):
            rows = jnp.where(lane // 32 == s, jnp.take_along_axis(parts[s], index, axis=1), rows)
        lead = rows.astype(jnp.bfloat16).astype(jnp.float32)
        rest = rows - lead
        for c in range(8):
            both = [jnp.broadcast_to(v[c : c + 1], (8, 128)) for v in (lead, rest)]
            pieces_ref[c, k] = jnp.concatenate(both, axis=0).astype(jnp.bfloat16)


def group_histogram(words_ref, pieces_ref, g, low, high):
    words = words_ref.at[pl.ds(pl.multiple_of(g * 8, 8), 8)]
    one = jnp.ones((16, 128), jnp.bfloat16)
    zero = jnp.zeros((16, 128), jnp.bfloat16)
    acc = jnp.zeros((128, 256), jnp.float32)
    for c in range(8):
        pieces = [pieces_ref[c, k] for k in range(4)]
        lhs_rows, rhs_rows = [], []
        for j in range(8):
            w = jnp.broadcast_to(words[pl.ds(j, 1), pl.ds(128 * c, 128)], (16, 128))
            halves = [w.astype(jnp.int16), (w >> 16).astype(jnp.int16)]
            lhs_cols, rhs_cols = [], []
            for k in range(4):
                b = k % 2
                l = halves[k // 2] & jnp.int16(31 << (8 * b))
                h = halves[k // 2] & jnp.int16(np.array(224 << (8 * b), np.uint16).astype(np.int16))
                lhs_cols.append(jnp.where(h == high[b], pieces[k], zero))
                rhs_cols.append(jnp.concatenate([jnp.where(l == low[b][p], one, zero) for p in range(2)], axis=0))
            lhs_rows.append(jnp.concatenate(lhs_cols, axis=1))
            rhs_rows.append(jnp.concatenate(rhs_cols, axis=1))
        lhs = jnp.concatenate(lhs_rows, axis=0)
        rhs = jnp.concatenate(rhs_rows, axis=0).astype(jnp.float8_e4m3fn)
        acc = acc + lax.dot_general(lhs, rhs, (((1,), (1,)), ((), ())), preferred_element_type=jnp.float32)
    block = lax.broadcasted_iota(jnp.int32, (8, 256), 1) // 32
    out = jnp.zeros((8, 256), jnp.float32)
    for j in range(8):
        out = out + jnp.where(block == j, acc[16 * j : 16 * j + 8] + acc[16 * j + 8 : 16 * j + 16], 0.0)
    return out


def three_pieces(v):
    a = v.astype(jnp.bfloat16)
    v = v - a.astype(jnp.float32)
    b = v.astype(jnp.bfloat16)
    v = v - b.astype(jnp.float32)
    return [a, b, v.astype(jnp.bfloat16)]


def cut_positions(hist, thresholds):
    sub = lax.broadcasted_iota(jnp.int32, (8, 256), 0)
    block = lax.broadcasted_iota(jnp.int32, (8, 256), 1) // 32
    upto = hist
    for shift in (1, 2, 4):
        upto = upto + jnp.where(sub >= shift, pltpu.roll(upto, shift, 0), 0.0)
    above = jnp.where(sub >= 1, pltpu.roll(upto, 1, 0), 0.0)

    def diagonal(v):
        rows = jnp.concatenate([jnp.where(block == f, v, 0.0) for f in range(8)], axis=0)
        return jnp.concatenate(three_pieces(rows), axis=1)

    rhs = jnp.concatenate([diagonal(hist), diagonal(above)], axis=1)
    l_out = lax.broadcasted_iota(jnp.int32, (32, 256), 0)
    l_in = lax.broadcasted_iota(jnp.int32, (32, 256), 1) % 32
    earlier = (l_in < l_out).astype(jnp.float32).astype(jnp.bfloat16)
    same = (l_in == l_out).astype(jnp.float32).astype(jnp.bfloat16)
    ones = jnp.ones((32, 256), jnp.bfloat16)
    lhs = jnp.concatenate(
        [
            jnp.concatenate([earlier] * 3 + [ones] * 3, axis=1),
            jnp.concatenate([same] * 3 + [jnp.zeros_like(ones)] * 3, axis=1),
        ],
        axis=0,
    )
    out = lax.dot_general(lhs, rhs, (((1,), (1,)), ((), ())), preferred_element_type=jnp.float32)
    before, own = out[:32], out[32:]
    scale = 1.0 / (own + 1.0)
    last = before[31:32] + own[31:32]
    rows = []
    for f in range(8):
        target = thresholds * last[:, 8 * f + 7 : 8 * f + 8]
        part = jnp.zeros((32, 128), jnp.float32)
        for h in range(8):
            col = 8 * f + h
            ratio = (target - before[:, col : col + 1]) * scale[:, col : col + 1]
            part = part + jnp.clip(ratio, 0.0, 1.0)
        rows.append(jnp.sum(part, axis=0, keepdims=True))
    return jnp.concatenate(rows, axis=0)


def kernel(
    bins_ref, h_ref, t_ref, o_ref,
    raw, words, pieces, sent, got, swap_out, swap_in, own_cuts, cuts,
    load_sem, send_sem, recv_sem, swap_send, swap_recv, cut_send, cut_recv,
):
    r = lax.axis_index("rows")
    feat = lax.axis_index("feat")
    core = r % 2
    y = (r // 2) % 4
    z = (r // 8) % 2
    x = r // 16
    chip = x * 4 + y

    def device(dx, dy, c):
        return (row_of((x + dx) % 4, z, (y + dy) % 4, c), feat)

    partner = (row_of(x, 1 - z, y, 1), feat)
    mesh_ids = dict(device_id_type=pl.DeviceIdType.MESH)

    loads = [
        pltpu.make_async_copy(bins_ref.at[pl.ds(128 * c, 128)], raw.at[pl.ds(128 * c, 128)], load_sem.at[c])
        for c in range(8)
    ]
    for load in loads:
        load.start()

    barrier = pltpu.get_barrier_semaphore()
    for dx, dy in OFFSETS[:-1]:
        pl.semaphore_signal(barrier, inc=1, device_id=device(dx, dy, 1), **mesh_ids)

    @pl.when(core == 0)
    def _():
        pl.semaphore_signal(barrier, inc=1, device_id=device(0, 0, 1), **mesh_ids)

    @pl.when(core == 1)
    def _():
        for dx, dy in OFFSETS:
            pl.semaphore_signal(barrier, inc=1, device_id=device(dx, dy, 0), **mesh_ids)
        pl.semaphore_signal(barrier, inc=1, device_id=partner, **mesh_ids)

    low, high = digit_patterns()
    spread_weights(h_ref, pieces)
    for c in range(8):
        loads[c].wait()
        words[:, pl.ds(128 * c, 128)] = raw[pl.ds(128 * c, 128), :].T

    def send(s):
        dx, dy = OFFSETS[s]
        return pltpu.make_async_remote_copy(
            src_ref=sent.at[s], dst_ref=got.at[2 * chip + core], send_sem=send_sem, recv_sem=recv_sem,
            device_id=device(dx, dy, 1), **mesh_ids,
        )

    for s in range(15):
        dx, dy = OFFSETS[s]
        g = ((x + dx) % 4) * 4 + (y + dy) % 4
        sent[s] = group_histogram(words, pieces, g, low, high)
        if s == BARRIER_STEP:

            @pl.when(core == 0)
            def _():
                pl.semaphore_wait(barrier, 16)

            @pl.when(core == 1)
            def _():
                pl.semaphore_wait(barrier, 32)

            for e in range(s):
                send(e).start()
        if s >= BARRIER_STEP:
            send(s).start()

    sent[15] = group_histogram(words, pieces, chip, low, high)

    @pl.when(core == 0)
    def _():
        send(15).start()

    def cut_copy(dx, dy, c):
        return pltpu.make_async_remote_copy(
            src_ref=own_cuts, dst_ref=cuts.at[chip], send_sem=cut_send, recv_sem=cut_recv,
            device_id=device(dx, dy, c), **mesh_ids,
        )

    def wait_all(ref, count, sem):
        part = ref.at[pl.ds(0, count)]
        pltpu.make_async_copy(part, part, sem).wait()

    @pl.when(core == 1)
    def _():
        got[2 * chip + 1] = sent[15]
        wait_all(got, 31, recv_sem)
        sums = [got[i] for i in range(32)]
        while len(sums) > 1:
            sums = [a + b for a, b in zip(sums[::2], sums[1::2])]
        swap_out[...] = sums[0]
        swap = pltpu.make_async_remote_copy(
            src_ref=swap_out, dst_ref=swap_in, send_sem=swap_send, recv_sem=swap_recv,
            device_id=partner, **mesh_ids,
        )
        swap.start()
        swap.wait()
        mine = cut_positions(sums[0] + swap_in[...], t_ref[...])
        own_cuts[...] = mine
        for dx, dy in OFFSETS[:-1]:
            for c in range(2):
                cut_copy(dx, dy, c).start()
        cut_copy(0, 0, 0).start()
        cuts[chip] = mine
        wait_all(cuts, 15, cut_recv)
        wait_all(sent, 15, send_sem)

    @pl.when(core == 0)
    def _():
        wait_all(cuts, 16, cut_recv)
        wait_all(sent, 16, send_sem)

    o_ref[...] = cuts[pl.ds(0, 16)].reshape(128, 128)

    @pl.when(core == 1)
    def _():
        wait_all(cuts, 31, cut_send)


def sketch(bins, hessian, thresholds):
    return pl.pallas_call(
        kernel,
        out_shape=jax.ShapeDtypeStruct((128, 128), jnp.float32),
        in_specs=[
            pl.BlockSpec(memory_space=pl.ANY),
            pl.BlockSpec(memory_space=pltpu.VMEM),
            pl.BlockSpec(memory_space=pltpu.VMEM),
        ],
        out_specs=pl.BlockSpec(memory_space=pltpu.VMEM),
        scratch_shapes=[
            pltpu.VMEM((1024, 128), jnp.int32),
            pltpu.VMEM((128, 1024), jnp.int32),
            pltpu.VMEM((8, 4, 16, 128), jnp.bfloat16),
            pltpu.VMEM((16, 8, 256), jnp.float32),
            pltpu.VMEM((32, 8, 256), jnp.float32),
            pltpu.VMEM((8, 256), jnp.float32),
            pltpu.VMEM((8, 256), jnp.float32),
            pltpu.VMEM((8, 128), jnp.float32),
            pltpu.VMEM((31, 8, 128), jnp.float32),
            pltpu.SemaphoreType.DMA((8,)),
            pltpu.SemaphoreType.DMA,
            pltpu.SemaphoreType.DMA,
            pltpu.SemaphoreType.DMA,
            pltpu.SemaphoreType.DMA,
            pltpu.SemaphoreType.DMA,
            pltpu.SemaphoreType.DMA,
        ],
        compiler_params=pltpu.CompilerParams(collective_id=0, has_side_effects=True),
        name="sketch",
    )(bins, hessian.reshape(32, 128), thresholds.reshape(1, 128))


def solution(mesh):
    in_specs = (P("rows", "feat"), P("rows"), P())
    out_specs = P("feat", None)
    return jax.shard_map(sketch, mesh=mesh, in_specs=in_specs, out_specs=out_specs, check_vma=False)
```

```python
import functools

import jax
import jax.numpy as jnp
import numpy as np
from jax import lax
from jax.experimental import pallas as pl
from jax.experimental.pallas import tpu as pltpu
from jax.sharding import PartitionSpec as P

OFFSETS = sorted(
    ((dx, dy) for dx in range(4) for dy in range(4)),
    key=lambda o: -(min(o[0], 4 - o[0]) + min(o[1], 4 - o[1])),
)
X_ORDER = (2, 1, 3, 0)
BARRIER_STEP = 7
BATCHES = {7: ((0, 0, 4), (1, 0, 4)), 9: ((2, 0, 2),), 11: ((2, 2, 2),)}
FINISH_AT = 3
F8 = jnp.float8_e4m3fn


def row_of(x, z, y, core):
    return ((x * 2 + z) * 4 + y) * 2 + core


def digit_patterns():
    r = lax.broadcasted_iota(jnp.int32, (32, 128), 0)
    low = [(r << (8 * b)).astype(jnp.int16) for b in range(2)]
    high = [((r[:16] % 8) << (5 + 8 * b)).astype(jnp.int16) for b in range(2)]
    return low, high


def spread_weights(h_ref, pieces_ref):
    lane = lax.broadcasted_iota(jnp.int32, (8, 128), 1)
    parts = [h_ref[pl.ds(s, 8, stride=4), :] for s in range(4)]
    for k in range(4):
        index = (lane % 32) * 4 + k
        rows = jnp.zeros((8, 128), jnp.float32)
        for s in range(4):
            rows = jnp.where(lane // 32 == s, jnp.take_along_axis(parts[s], index, axis=1), rows)
        lead = rows.astype(jnp.bfloat16).astype(jnp.float32)
        rest = rows - lead
        for c in range(8):
            both = [jnp.broadcast_to(v[c : c + 1], (8, 128)) for v in (lead, rest)]
            pieces_ref[c, k] = jnp.concatenate(both, axis=0).astype(jnp.bfloat16)


def group_chunk(words_ref, pieces_ref, g, c, low, high, accs):
    words = words_ref.at[pl.ds(pl.multiple_of(g * 8, 8), 8)]
    zero = jnp.zeros((16, 128), jnp.bfloat16)
    one8 = jnp.ones((32, 128), F8)
    zero8 = jnp.zeros((32, 128), F8)
    halves = []
    for j in range(8):
        w = jnp.broadcast_to(words[pl.ds(j, 1), pl.ds(128 * c, 128)], (16, 128))
        halves.append([w.astype(jnp.int16), (w >> 16).astype(jnp.int16)])
    for q in range(2):
        lhs_rows, rhs_rows = [], []
        for j in range(8):
            lhs_cols, rhs_cols = [], []
            for b in range(2):
                l = halves[j][q] & jnp.int16(31 << (8 * b))
                h = halves[j][q] & jnp.int16(np.array(224 << (8 * b), np.uint16).astype(np.int16))
                lhs_cols.append(jnp.where(h == high[b], pieces_ref[c, 2 * q + b], zero))
                rhs_cols.append(jnp.where(jnp.concatenate([l, l], axis=0) == low[b], one8, zero8))
            lhs_rows.append(jnp.concatenate(lhs_cols, axis=1))
            rhs_rows.append(jnp.concatenate(rhs_cols, axis=1))
        pltpu.matmul_push_rhs(jnp.concatenate(rhs_rows, axis=0), staging_register=c % 2, mxu_index=q, transpose=True)
        pltpu.matmul_acc_lhs(accs[q], jnp.concatenate(lhs_rows, axis=0), load_staged_rhs=c % 2)


def group_result(accs):
    a, b = (pltpu.matmul_pop(acc) for acc in accs)
    block = lax.broadcasted_iota(jnp.int32, (8, 256), 1) // 32
    out = None
    for j in range(8):
        lead, rest = slice(16 * j, 16 * j + 8), slice(16 * j + 8, 16 * j + 16)
        own = (a[lead] + b[lead]) + (a[rest] + b[rest])
        out = own if j == 0 else jnp.where(block == j, own, out)
    return out


def three_pieces(v):
    a = v.astype(jnp.bfloat16)
    v = v - a.astype(jnp.float32)
    b = v.astype(jnp.bfloat16)
    v = v - b.astype(jnp.float32)
    return [a, b, v.astype(jnp.bfloat16)]


def prefix_matrix():
    l_out = lax.broadcasted_iota(jnp.int32, (32, 256), 0)
    l_in = lax.broadcasted_iota(jnp.int32, (32, 256), 1) % 32
    both = jnp.concatenate([l_in < l_out, l_in == l_out], axis=0)
    return both.astype(jnp.float32).astype(jnp.bfloat16)


def cut_positions(hist, thresholds, prefix, accs):
    sub = lax.broadcasted_iota(jnp.int32, (8, 256), 0)
    block = lax.broadcasted_iota(jnp.int32, (8, 256), 1) // 32
    upto = hist
    for shift in (1, 2, 4):
        upto = upto + jnp.where(sub >= shift, pltpu.roll(upto, shift, 0), 0.0)
    above = jnp.where(sub >= 1, pltpu.roll(upto, 1, 0), 0.0)

    def times_diagonal(q, lhs, v):
        rows = jnp.concatenate([jnp.where(block == f, v, 0.0) for f in range(8)], axis=0)
        rhs = jnp.concatenate([*three_pieces(rows), jnp.zeros((64, 256), jnp.bfloat16)], axis=0)
        pltpu.matmul_push_rhs(rhs, staging_register=0, mxu_index=q, transpose=True)
        pltpu.matmul_acc_lhs(accs[q], lhs, load_staged_rhs=0)

    def joined(v):
        return (v[:, :128] + pltpu.roll(v[:, :128], 64, 1)) + v[:, 128:]

    times_diagonal(0, prefix, hist)
    times_diagonal(1, jnp.ones((16, 256), jnp.bfloat16), above)
    out = joined(pltpu.matmul_pop(accs[0]))
    out_above = joined(pltpu.matmul_pop(accs[1])[:8])
    before = out[:32] + jnp.concatenate([out_above] * 4, axis=0)
    own = out[32:]
    scale = 1.0 / (own + 1.0)
    last = before[31:32] + own[31:32]
    rows = []
    for f in range(8):
        target = thresholds * last[:, 8 * f + 7 : 8 * f + 8]
        part = jnp.zeros((32, 128), jnp.float32)
        for h in range(8):
            col = 8 * f + h
            ratio = (target - before[:, col : col + 1]) * scale[:, col : col + 1]
            part = part + jnp.clip(ratio, 0.0, 1.0)
        rows.append(jnp.sum(part, axis=0, keepdims=True))
    return jnp.concatenate(rows, axis=0)


def body(
    accs,
    bins_ref, h_hbm, t_hbm, o_ref,
    h_ref, t_ref, raw, words, pieces, prefix, sent, got, part_out, part_in, own_cuts, cuts,
    load_sem, send_sem, recv_sem, part_send, part_recv, cut_send, cut_recv, ready,
):
    r = lax.axis_index("rows")
    feat = lax.axis_index("feat")
    core = r % 2
    y = (r // 2) % 4
    z = (r // 8) % 2
    x = r // 16
    chip = x * 4 + y
    mesh_ids = dict(device_id_type=pl.DeviceIdType.MESH)

    def device(dx, dy, c, dz=0):
        return (row_of((x + dx) % 4, (z + dz) % 2, (y + dy) % 4, c), feat)

    weights_load = pltpu.make_async_copy(h_hbm, h_ref, load_sem.at[8])
    thresholds_load = pltpu.make_async_copy(t_hbm, t_ref, load_sem.at[9])
    loads = [
        pltpu.make_async_copy(bins_ref.at[pl.ds(128 * c, 128)], raw.at[pl.ds(128 * c, 128)], load_sem.at[c])
        for c in range(8)
    ]
    weights_load.start()
    for load in loads:
        load.start()
    thresholds_load.start()

    barrier = pltpu.get_barrier_semaphore()
    for dx in X_ORDER[:3]:
        pl.semaphore_signal(barrier, inc=1, device_id=device(dx, 0, 1), **mesh_ids)

    @pl.when(core == 0)
    def _():
        pl.semaphore_signal(barrier, inc=1, device_id=device(0, 0, 1), **mesh_ids)

    @pl.when(core == 1)
    def _():
        for dz in (1, 0):
            for dy in X_ORDER:
                if dy or dz:
                    pl.semaphore_signal(barrier, inc=1, device_id=device(0, dy, 0, dz), **mesh_ids)

    low, high = digit_patterns()
    prefix[...] = prefix_matrix()
    weights_load.wait()
    spread_weights(h_ref, pieces)
    for c in range(8):
        loads[c].wait()
        words[:, pl.ds(128 * c, 128)] = raw[pl.ds(128 * c, 128), :].T
    thresholds_load.wait()

    def send(place, first, count):
        return pltpu.make_async_remote_copy(
            src_ref=sent.at[place, pl.ds(first, count)],
            dst_ref=got.at[2 * x + core, pl.ds(first, count)],
            send_sem=send_sem, recv_sem=recv_sem, device_id=device(X_ORDER[place], 0, 1), **mesh_ids,
        )

    def finish(s, accs):
        sent[s // 4, s % 4] = group_result(accs)
        if s == BARRIER_STEP:

            @pl.when(core == 1)
            def _():
                pl.semaphore_wait(barrier, 7)
                pl.semaphore_signal(ready, inc=1, device_id=device(0, 0, 0), **mesh_ids)

            @pl.when(core == 0)
            def _():
                pl.semaphore_wait(ready, 1)

        for batch in BATCHES.get(s, ()):
            send(*batch).start()

    pairs, cut_accs = (accs[:2], accs[2:4]), accs[4:]
    for acc in accs:
        pltpu.matmul_pop(acc)
    for s in range(16):
        g = ((x + X_ORDER[s // 4]) % 4) * 4 + s % 4
        for c in range(8):
            group_chunk(words, pieces, g, c, low, high, pairs[s % 2])
            if c + 1 == FINISH_AT and s:
                finish(s - 1, pairs[(s - 1) % 2])
    finish(15, pairs[1])

    def part_copy(dy, dz):
        return pltpu.make_async_remote_copy(
            src_ref=part_out.at[(y + dy) % 4], dst_ref=part_in.at[4 * z + y],
            send_sem=part_send, recv_sem=part_recv, device_id=device(0, dy, 1, dz), **mesh_ids,
        )

    def cut_copy(dx, dy, c):
        return pltpu.make_async_remote_copy(
            src_ref=own_cuts, dst_ref=cuts.at[chip], send_sem=cut_send, recv_sem=cut_recv,
            device_id=device(dx, dy, c), **mesh_ids,
        )

    def wait_all(ref, count, sem):
        whole = ref.at[pl.ds(0, count)]
        pltpu.make_async_copy(whole, whole, sem).wait()

    def tree_sum(terms):
        while len(terms) > 1:
            terms = [a + b for a, b in zip(terms[::2], terms[1::2])]
        return terms[0]

    @pl.when(core == 0)
    def _():
        send(3, 0, 4).start()
        pl.semaphore_wait(barrier, 7)
        pl.semaphore_signal(ready, inc=1, device_id=device(0, 0, 1), **mesh_ids)
        wait_all(cuts, 16, cut_recv)
        wait_all(sent, 4, send_sem)

    @pl.when(core == 1)
    def _():
        got[2 * x + 1] = sent[3]
        wait_all(got, 7, recv_sem)
        pl.semaphore_wait(ready, 1)
        for yy in range(4):
            part_out[yy] = tree_sum([got[i, yy] for i in range(8)])
        for dz in (1, 0):
            for dy in X_ORDER:
                if dy or dz:
                    part_copy(dy, dz).start()
        part_in[4 * z + y] = part_out[y]
        wait_all(part_in, 7, part_recv)
        hist = tree_sum([part_in[i] for i in range(8)])
        mine = cut_positions(hist, t_ref[...], prefix[...], cut_accs)
        own_cuts[...] = mine
        for dx, dy in OFFSETS[:-1]:
            for c in range(2):
                cut_copy(dx, dy, c).start()
        cut_copy(0, 0, 0).start()
        cuts[chip] = mine
        wait_all(sent, 3, send_sem)
        wait_all(part_in, 7, part_send)
        wait_all(cuts, 15, cut_recv)
        wait_all(cuts, 31, cut_send)

    o_ref[...] = cuts[pl.ds(0, 16)].reshape(128, 128)


def kernel(*refs):
    group = [pltpu.ACC(q)((128, 256), jnp.float32) for q in range(2)]
    cut = [pltpu.ACC(0)((64, 256), jnp.float32), pltpu.ACC(1)((16, 256), jnp.float32)]
    pl.run_scoped(lambda *accs: body(accs, *refs), *group, *group, *cut)


def sketch(bins, hessian, thresholds):
    dma = pltpu.SemaphoreType.DMA
    f32 = jnp.float32
    return pl.pallas_call(
        kernel,
        out_shape=pltpu.VMEM((128, 128), f32),
        in_specs=[pl.BlockSpec(memory_space=pl.ANY)] * 3,
        out_specs=pl.BlockSpec(memory_space=pltpu.VMEM),
        scratch_shapes=[
            pltpu.VMEM((32, 128), f32),
            pltpu.VMEM((1, 128), f32),
            pltpu.VMEM((1024, 128), jnp.int32),
            pltpu.VMEM((128, 1024), jnp.int32),
            pltpu.VMEM((8, 4, 16, 128), jnp.bfloat16),
            pltpu.VMEM((64, 256), jnp.bfloat16),
            pltpu.VMEM((4, 4, 8, 256), f32),
            pltpu.VMEM((8, 4, 8, 256), f32),
            pltpu.VMEM((4, 8, 256), f32),
            pltpu.VMEM((8, 8, 256), f32),
            pltpu.VMEM((8, 128), f32),
            pltpu.VMEM((31, 8, 128), f32),
            dma((10,)),
            dma, dma, dma, dma, dma, dma,
            pltpu.SemaphoreType.REGULAR,
        ],
        compiler_params=pltpu.CompilerParams(collective_id=0, has_side_effects=True),
        name="sketch",
    )(bins, hessian.reshape(32, 128), thresholds.reshape(1, 128))


def solution(mesh):
    in_specs = (P("rows", "feat"), P("rows"), P())
    out_specs = P("feat", None)
    return jax.shard_map(sketch, mesh=mesh, in_specs=in_specs, out_specs=out_specs, check_vma=False)
```
